32 devices in a mesh: blk: 8 (over y, x, core), uly: 1, dp: 4 (over z).
Axes of the slice: x: 2, y: 2, z: 4, core: 2. Of those that a mesh axis runs over, the one named last changes fastest.
Arguments:
- short_tokens: bfloat16 [32, 1024, 4096], P(('blk', 'dp'), 'uly'), may hold values from -150 to 150, as said below
- short_segments: int32 [32, 1024], P(('blk', 'dp')), may hold values from 0 to 3, never falling along the last dimension, each value on 1 to 512 neighbouring positions
- long_tokens: bfloat16 [4, 3072, 4096], P('dp', 'blk'), may hold values from -150 to 150, as said below
- long_lengths: int32 [4], P('dp'), may hold values from 768 to 3072
- w_query: bfloat16 [4096, 2048], P(('blk', 'dp'), 'uly'), may hold values from -0.09375 to 0.09375
- w_key: bfloat16 [4096, 512], P(('blk', 'dp'), 'uly'), may hold values from -0.09375 to 0.09375
- w_value: bfloat16 [4096, 512], P(('blk', 'dp'), 'uly'), may hold values from -0.09375 to 0.09375
Outputs:
- short_out: bfloat16 [32, 1024, 2048], P(('blk', 'dp'), 'uly')
- long_out: bfloat16 [4, 3072, 2048], P('dp', 'blk', 'uly')
The draws below stay inside these ranges and needn't reach their ends.
Inputs may be any that keep to these rules, and one draw needn't show every extreme that they name: `short_tokens`: activations of the short bucket. `long_tokens`: activations of the long bucket; rows at or after a sequence's length are padding. `short_segments`: document numbers never fall along a sequence. `long_lengths`: a long sequence occupies positions 0 to its length - 1 of its 3072 slots.
All inputs are finite; a program needn't handle non-finite values.
Results may differ from the reference program's by a relative error of at most 0.012.
The reference program's roundings to bfloat16 on the way count: a program that leaves them out, or rounds other values in their place, can miss the bound.
Values may be sent and summed in bfloat16 or wider, within the bound.
A program may use at most 128 MiB of HBM per device.

```python
import math
import jax
import jax.numpy as jnp
import numpy as np
from jax import lax

D = 4096
HQ = 16
HK = 4
HD = 128
LS = 1024
NS = 32
NL = 4
LL = 3072


def token_rows(key, shape):
    base = jnp.clip(jax.random.normal(key, shape, jnp.float32), -6.0, 6.0)
    return base.astype(jnp.bfloat16)


def draw_short_tokens(key, part):
    return token_rows(jax.random.fold_in(key, 101), (NS, LS, D))


def draw_long_tokens(key, part):
    return token_rows(jax.random.fold_in(key, 202), (NL, LL, D))


def plant(values, stream_key, low, largest):
    place = [jax.random.randint(jax.random.fold_in(stream_key, axis), (), 0, length) for axis, length in enumerate(values.shape)]
    longest = values.shape.index(max(values.shape))
    neighbour = place[:longest] + [(place[longest] + 1) % values.shape[longest]] + place[longest + 1:]
    return values.at[tuple(place)].set(low).at[tuple(neighbour)].set(largest)


def levels(rng, dims, shards, least, top_value):
    def one(dim, blocks):
        heights = jax.random.uniform(jax.random.fold_in(jax.random.fold_in(rng, 6), dim), (blocks,), jnp.float32, least / len(shards), top_value / len(shards))
        return jnp.repeat(jnp.exp(heights), dims[dim] // blocks).reshape((-1,) + (1,) * (len(dims) - dim - 1))

    loudness = one(*shards[0])
    for cut in shards[1:]:
        loudness = loudness * one(*cut)
    return loudness


def length_profile(number_of, total, most, lean):
    weights = [(1 << 20) // math.isqrt(grade ** lean) + 1 for grade in range(2, number_of + 1)]
    spare, counts = total - most - (number_of - 1), [1] * (number_of - 1)
    while spare > 0:
        movable = [i for i in range(number_of - 1) if counts[i] < most]
        whole, remaining = sum([weights[i] for i in movable]), spare
        for i in movable:
            extra = min(most - counts[i], max(1, remaining * weights[i] // whole), spare)
            counts[i] = counts[i] + extra
            spare = spare - extra
    return np.array([most] + counts)


def uneven(own_key, number_of, total, most, lean):
    if number_of == 2:
        one = jax.random.randint(own_key, (), max(1, total - most), min(most, total - 1) + 1)
        return jnp.stack([one, total - one])
    lengths = jnp.asarray(length_profile(number_of, total, most, lean), jnp.int32)
    twos = (number_of - 1) // 2
    donor, receiver = lengths[1:1 + 2 * twos:2], lengths[2:2 + 2 * twos:2]
    room = jnp.minimum(donor - 1, most - receiver)
    shifted = jax.random.randint(jax.random.fold_in(own_key, 1), (twos,), 0, 1 << 20) % (room + 1)
    lengths = lengths.at[1:1 + 2 * twos:2].set(donor - shifted).at[2:2 + 2 * twos:2].set(receiver + shifted)
    return lengths[jax.random.permutation(jax.random.fold_in(own_key, 2), number_of)]


def gaussian(own_key, extent, width, bound, split=(), kind=jnp.bfloat16):
    factor_of = levels(own_key, extent, split, -0.22, 0.18) if split else 1.0
    drawn = jax.random.normal(own_key, extent, jnp.float32) * width * factor_of
    return jnp.minimum(jnp.maximum(drawn, -bound), bound).astype(kind)


def setup_inputs(seed: int = 0) -> dict:
    keys = jax.random.split(jax.random.key(seed), 8)
    short_tokens = draw_short_tokens(jax.random.fold_in(keys[7], 71), 0)
    short_segments = jax.vmap(lambda own: jnp.searchsorted(jnp.cumsum(uneven(own, 4, LS, LS // 2, 1)), jnp.arange(LS), side="right"))(jax.random.split(keys[1], NS)).reshape((NS, LS)).astype(jnp.int32)
    long_tokens = draw_long_tokens(jax.random.fold_in(keys[7], 71), 0)
    long_lengths = plant(jax.random.randint(keys[3], (NL,), LL // 4, LL + 1), jax.random.fold_in(keys[3], 1), LL // 4, LL).astype(jnp.int32)
    w_query = gaussian(keys[4], (D, HQ * HD), D ** -0.5, 0.09375, ((0, 32),))
    w_key = gaussian(keys[5], (D, HK * HD), D ** -0.5, 0.09375, ((0, 32),))
    w_value = gaussian(keys[6], (D, HK * HD), D ** -0.5, 0.09375, ((0, 32),))
    return {"short_tokens": short_tokens, "short_segments": short_segments, "long_tokens": long_tokens, "long_lengths": long_lengths, "w_query": w_query, "w_key": w_key, "w_value": w_value}


masked_score = -1e+30

def rounded_wide(array):
    return lax.optimization_barrier(array.astype(jnp.bfloat16)).astype(jnp.float32)

def project(rows, weight):
    return jnp.dot(rows, weight, preferred_element_type=jnp.float32)

def attention(queries, key_rows, value_rows, visible_rows):
    seq_len = key_rows.shape[0]
    block_rows = min(512, seq_len)
    group_size = HQ // HK
    key_heads = key_rows.reshape(seq_len, HK, HD)
    value_heads = value_rows.reshape(seq_len, HK, HD)
    outputs = []
    for block_index in range(seq_len // block_rows):
        first_row = block_index * block_rows
        query_heads = queries[first_row:first_row + block_rows].reshape(block_rows, HK, group_size, HD)
        visible = visible_rows(first_row, block_rows)
        scores = jnp.einsum('bhgd,khd->hgbk', query_heads, key_heads) * (1.0 / math.sqrt(HD))
        scores = jnp.where(visible, scores, masked_score)
        row_max = lax.optimization_barrier(jnp.max(scores, axis=-1, keepdims=True))
        exponentials = jnp.where(visible, jnp.exp(scores - row_max), 0.0)
        totals = lax.optimization_barrier(jnp.sum(exponentials, axis=-1))
        mixed = jnp.einsum('hgbk,khd->hgbd', rounded_wide(exponentials), value_heads)
        mixed = mixed / totals[..., None]
        outputs.append(jnp.transpose(mixed, (2, 0, 1, 3)).reshape(block_rows, HQ * HD))
    return jnp.concatenate(outputs, axis=0)

def reference(short_tokens, short_segments, long_tokens, long_lengths, w_query, w_key, w_value):

    def one_short(inputs):
        rows, segments = inputs
        queries = rounded_wide(project(rows, w_query))
        key_rows = rounded_wide(project(rows, w_key))
        value_rows = rounded_wide(project(rows, w_value))
        positions = jnp.arange(rows.shape[0], dtype=jnp.int32)

        def visible_rows(first_row, block_rows):
            query_pos = positions[first_row:first_row + block_rows]
            query_seg = segments[first_row:first_row + block_rows]
            return (positions[None, :] <= query_pos[:, None]) & (segments[None, :] == query_seg[:, None])
        mixed = attention(queries, key_rows, value_rows, visible_rows)
        return mixed.astype(jnp.bfloat16)

    def one_long(inputs):
        rows, length = inputs
        queries = rounded_wide(project(rows, w_query))
        key_rows = rounded_wide(project(rows, w_key))
        value_rows = rounded_wide(project(rows, w_value))
        positions = jnp.arange(rows.shape[0], dtype=jnp.int32)

        def visible_rows(first_row, block_rows):
            query_pos = positions[first_row:first_row + block_rows]
            return (positions[None, :] <= query_pos[:, None]) & (positions[None, :] < length)
        mixed = attention(queries, key_rows, value_rows, visible_rows)
        mixed = jnp.where(positions[:, None] < length, mixed, 0.0)
        return mixed.astype(jnp.bfloat16)
    short_out = lax.map(one_short, (short_tokens, short_segments))
    long_out = lax.map(one_long, (long_tokens, long_lengths))
    return (short_out, long_out)
```

```python
import functools
import math

import jax
import jax.numpy as jnp
from jax import lax
from jax.experimental import pallas as pl
from jax.experimental.pallas import tpu as pltpu
from jax.sharding import PartitionSpec as P

HD = 128
LONGEST_DOCUMENT = 512

masked_score = -1e30
exp2_factor = math.log2(math.e) / math.sqrt(HD)


def raw_scores(queries, keys):
    return lax.dot_general(
        queries, keys, (((1,), (1,)), ((), ())), preferred_element_type=jnp.float32
    )


def short_kernel(block_rows, col_ref, row_ref, q_ref, k_ref, v_ref, out_ref, bias_ref):
    seq_len = q_ref.shape[0]

    def window(first_row):
        return max(0, first_row - LONGEST_DOCUMENT), first_row + block_rows

    @pl.when(pl.program_id(0) == 0)
    def _():
        for first_row in range(0, seq_len, block_rows):
            low, high = window(first_row)
            shape = (block_rows, high - low)
            query_pos = first_row + lax.broadcasted_iota(jnp.int32, shape, 0)
            key_pos = low + lax.broadcasted_iota(jnp.int32, shape, 1)
            visible = (key_pos <= query_pos) & (
                col_ref[first_row : first_row + block_rows, :] == row_ref[:, low:high]
            )
            bias_ref[first_row : first_row + block_rows, low:high] = jnp.where(
                visible, 0.0, masked_score
            )

    for first_row in range(0, seq_len, block_rows):
        low, high = window(first_row)
        rows = slice(first_row, first_row + block_rows)
        scores = raw_scores(q_ref[rows, :], k_ref[low:high, :]) + bias_ref[rows, low:high]
        row_max = jnp.max(scores, axis=-1, keepdims=True)
        exponentials = jnp.exp2((scores - row_max) * exp2_factor)
        totals = jnp.sum(exponentials, axis=-1, keepdims=True)
        mixed = jnp.dot(
            exponentials.astype(jnp.bfloat16),
            v_ref[low:high, :],
            preferred_element_type=jnp.float32,
        )
        out_ref[rows, :] = (mixed / totals).astype(jnp.bfloat16)


def short_attention(projected, segments, heads, kv_heads):
    seq_len = projected.shape[0]
    group = heads // kv_heads
    block_rows = math.gcd(seq_len, 256)
    return pl.pallas_call(
        functools.partial(short_kernel, block_rows),
        grid=(heads,),
        in_specs=[
            pl.BlockSpec((seq_len, 1), lambda h: (0, 0)),
            pl.BlockSpec((1, seq_len), lambda h: (0, 0)),
            pl.BlockSpec((seq_len, HD), lambda h: (0, h)),
            pl.BlockSpec((seq_len, HD), lambda h: (0, heads + h // group)),
            pl.BlockSpec((seq_len, HD), lambda h: (0, heads + kv_heads + h // group)),
        ],
        out_specs=pl.BlockSpec((seq_len, HD), lambda h: (0, h)),
        out_shape=jax.ShapeDtypeStruct((seq_len, heads * HD), jnp.bfloat16),
        scratch_shapes=[pltpu.VMEM((seq_len, seq_len), jnp.float32)],
        cost_estimate=pl.CostEstimate(
            flops=4 * heads * seq_len * seq_len * HD,
            bytes_accessed=4 * seq_len * heads * HD,
            transcendentals=heads * seq_len * seq_len,
        ),
        compiler_params=pltpu.CompilerParams(dimension_semantics=("arbitrary",)),
    )(segments[:, None], segments[None, :], projected, projected, projected)


def long_kernel(key_rows, info_ref, q_ref, k_ref, v_ref, out_ref):
    long_count = q_ref.shape[0]
    first_pos = info_ref[0]
    long_len = info_ref[1]
    queries = q_ref[...]
    query_pos = first_pos + lax.broadcasted_iota(jnp.int32, (long_count, 1), 0)
    last_key = jnp.minimum(query_pos, long_len - 1)

    def update(block, states, masked):
        running_max, running_sum, accumulated = states
        start = pl.multiple_of(block * key_rows, key_rows)
        scores = raw_scores(queries, k_ref[pl.ds(start, key_rows), :])
        if masked:
            key_pos = start + lax.broadcasted_iota(jnp.int32, (long_count, key_rows), 1)
            scores = jnp.where(key_pos <= last_key, scores, masked_score)
        new_max = jnp.maximum(running_max, jnp.max(scores, axis=-1, keepdims=True))
        rescale = jnp.exp2((running_max - new_max) * exp2_factor)
        exponentials = jnp.exp2((scores - new_max) * exp2_factor)
        running_sum = running_sum * rescale + jnp.sum(exponentials, axis=-1, keepdims=True)
        accumulated = accumulated * rescale + jnp.dot(
            exponentials.astype(jnp.bfloat16),
            v_ref[pl.ds(start, key_rows), :],
            preferred_element_type=jnp.float32,
        )
        return new_max, running_sum, accumulated

    @pl.when(first_pos >= long_len)
    def _():
        out_ref[...] = jnp.zeros_like(out_ref)

    @pl.when(first_pos < long_len)
    def _():
        whole = jnp.minimum(first_pos + 1, long_len) // key_rows
        used = (jnp.minimum(first_pos + long_count, long_len) + key_rows - 1) // key_rows
        states = (
            jnp.full((long_count, 1), masked_score, jnp.float32),
            jnp.zeros((long_count, 1), jnp.float32),
            jnp.zeros((long_count, HD), jnp.float32),
        )
        states = lax.fori_loop(0, whole, lambda i, s: update(i, s, False), states)
        states = lax.fori_loop(whole, used, lambda i, s: update(i, s, True), states)
        running_max, running_sum, accumulated = states
        mixed = jnp.where(query_pos < long_len, accumulated / running_sum, 0.0)
        out_ref[...] = mixed.astype(jnp.bfloat16)


def long_attention(queries, kv_rows, first_pos, long_len, kv_heads):
    long_count = queries.shape[0]
    heads = queries.shape[1] // HD
    total_rows = kv_rows.shape[0]
    group = heads // kv_heads
    key_rows = math.gcd(total_rows, 768)
    return pl.pallas_call(
        functools.partial(long_kernel, key_rows),
        grid_spec=pltpu.PrefetchScalarGridSpec(
            num_scalar_prefetch=1,
            grid=(heads,),
            in_specs=[
                pl.BlockSpec((long_count, HD), lambda h, info: (0, h)),
                pl.BlockSpec((total_rows, HD), lambda h, info: (0, h // group)),
                pl.BlockSpec((total_rows, HD), lambda h, info: (0, kv_heads + h // group)),
            ],
            out_specs=pl.BlockSpec((long_count, HD), lambda h, info: (0, h)),
        ),
        out_shape=jax.ShapeDtypeStruct((long_count, heads * HD), jnp.bfloat16),
        cost_estimate=pl.CostEstimate(
            flops=4 * heads * long_count * total_rows * HD,
            bytes_accessed=4 * total_rows * kv_heads * HD,
            transcendentals=heads * long_count * total_rows,
        ),
        compiler_params=pltpu.CompilerParams(dimension_semantics=("arbitrary",)),
    )(jnp.stack([first_pos, long_len]), queries, kv_rows, kv_rows)


def project(rows, weight):
    return jnp.dot(rows, weight, preferred_element_type=jnp.float32).astype(jnp.bfloat16)


def local(short_tokens, short_segments, long_tokens, long_lengths, w_query, w_key, w_value):
    short_rows = short_tokens[0]
    long_rows = long_tokens[0]
    long_count = long_rows.shape[0]
    query_cols = w_query.shape[1]
    heads, kv_heads = query_cols // HD, w_key.shape[1] // HD
    weights = lax.all_gather(
        jnp.concatenate([w_query, w_key, w_value], axis=1), ("blk", "dp"), axis=0, tiled=True
    )
    kv_long = project(long_rows, weights[:, query_cols:])
    kv_whole = lax.all_gather(kv_long, "blk", axis=0, tiled=True)
    whole_rows = lax.all_gather(short_rows, "uly", axis=0, tiled=True)
    short_projected = project(whole_rows, weights)
    query_long = project(long_rows, weights[:, :query_cols])
    attended = short_attention(short_projected, short_segments[0], heads, kv_heads)
    short_back = lax.all_to_all(attended, "uly", split_axis=0, concat_axis=1, tiled=True)
    first_pos = lax.axis_index("blk").astype(jnp.int32) * long_count
    mixed = long_attention(query_long, kv_whole, first_pos, long_lengths[0], kv_heads)
    return short_back[None], mixed[None]


def solution(mesh):
    return jax.shard_map(
        local,
        mesh=mesh,
        in_specs=(
            P(("blk", "dp"), "uly", None),
            P(("blk", "dp"), None),
            P("dp", "blk", None),
            P("dp"),
            P(("blk", "dp"), "uly"),
            P(("blk", "dp"), "uly"),
            P(("blk", "dp"), "uly"),
        ),
        out_specs=(P(("blk", "dp"), "uly", None), P("dp", "blk", "uly")),
        check_vma=False,
    )
```
